512 devices in a mesh: ctx: 32 (over x, z_lo), tp: 16 (over y, z_hi, core).
Axes of the slice: x: 4, y: 4, z: 16 (z_hi: 2, z_lo: 8; z = z_hi * 8 + z_lo), core: 2. Of those that a mesh axis runs over, the one named last changes fastest.
Arguments:
- queries: bfloat16 [8192, 8192], P('ctx', 'tp'), may hold values from -8 to 8
- keys: bfloat16 [8192, 1024], P('ctx'), may hold values from -7 to 7
- values: bfloat16 [8192, 1024], P('ctx'), may hold values from -6 to 6
- out_weight: bfloat16 [8192, 4096], P('tp'), may hold values from -0.25 to 0.25
- block_order: int32 [64], P('ctx'), may hold values from 0 to 63, each once
Outputs:
- projected: bfloat16 [8192, 4096], P('ctx', 'tp')
The draws below stay inside these ranges and needn't reach their ends.
Inputs may be any that keep to these rules, and one draw needn't show every extreme that they name: `block_order`: every sequence block appears exactly once.
All inputs are finite; a program needn't handle non-finite values.
Results may differ from the reference program's by a relative error of at most 0.015.
Values may be sent and summed in bfloat16 or wider, within the bound.
A program may use at most 64 MiB of HBM per device.

```python
import math
import jax
import jax.numpy as jnp
from jax import lax

QUERY_HEADS = 64
KEY_VALUE_HEADS = 8
HEAD_SIZE = 128
DW = 4096
BLK = 128
SEQUENCE_TOKENS = 8192
NBLK = 64


def shared_vectors(key):
    key_random_keys = jax.random.fold_in(key, 11)
    key_queries = jax.random.fold_in(key, 12)
    key_collection = jnp.clip(jax.random.normal(key_random_keys, (SEQUENCE_TOKENS, KEY_VALUE_HEADS * HEAD_SIZE), jnp.float32), -6.0, 6.0)
    queryset = jnp.clip(2.5 * jax.random.normal(key_queries, (SEQUENCE_TOKENS, QUERY_HEADS * HEAD_SIZE), jnp.float32), -8.0, 8.0)
    return (key_collection.astype(jnp.bfloat16), queryset.astype(jnp.bfloat16))


def draw_queries(key, part):
    return shared_vectors(key)[1]


def draw_keys(key, part):
    return shared_vectors(key)[0]


def steps_of(key, shape, split, least, largest):
    def one(dim, parts):
        heights = jax.random.uniform(jax.random.fold_in(jax.random.fold_in(key, 6), dim), (parts,), jnp.float32, least / len(split), largest / len(split))
        return jnp.repeat(jnp.exp(heights), shape[dim] // parts).reshape((-1,) + (1,) * (len(shape) - dim - 1))

    gain = one(*split[0])
    for cut in split[1:]:
        gain = gain * one(*cut)
    return gain


def noise(key, extent, deviation, bound, cuts=(), kind=jnp.bfloat16):
    drawn = jax.random.normal(key, extent, jnp.float32) * deviation
    if len(cuts) > 0:
        drawn = steps_of(key, extent, cuts, -0.22, 0.18) * drawn
    return jnp.clip(drawn, min=-bound, max=bound).astype(kind)


def setup_inputs(seed: int = 0) -> dict:
    key_list = jax.random.split(jax.random.key(seed), 6)
    return {
        "queries": draw_queries(jax.random.fold_in(key_list[5], 71), 0),
        "keys": draw_keys(jax.random.fold_in(key_list[5], 71), 0),
        "values": noise(key_list[2], (SEQUENCE_TOKENS, KEY_VALUE_HEADS * HEAD_SIZE), 1.0, 6.0, ((0, 32),)),
        "out_weight": noise(key_list[3], (QUERY_HEADS * HEAD_SIZE, DW), (QUERY_HEADS * HEAD_SIZE // 16) ** -0.5, 0.25, ((0, 16),)),
        "block_order": jax.random.permutation(key_list[4], NBLK).astype(jnp.int32),
    }


def reference(queries, keys, values, out_weight, block_order):
    head_group = QUERY_HEADS // KEY_VALUE_HEADS
    offsets = jnp.arange(BLK, dtype=jnp.int32)
    positions = (block_order[:, None].astype(jnp.int32) * BLK + offsets[None, :]).reshape(-1)
    scale = 1.0 / math.sqrt(HEAD_SIZE)
    q_heads = jnp.transpose(queries.reshape(SEQUENCE_TOKENS, QUERY_HEADS, HEAD_SIZE), (1, 0, 2))
    key_head_rows = jnp.transpose(keys.reshape(SEQUENCE_TOKENS, KEY_VALUE_HEADS, HEAD_SIZE), (1, 0, 2))
    value_head_rows = jnp.transpose(values.reshape(SEQUENCE_TOKENS, KEY_VALUE_HEADS, HEAD_SIZE), (1, 0, 2))
    q_pos = positions.reshape(SEQUENCE_TOKENS // BLK, BLK)

    def one_head(head):
        k_rows = key_head_rows[head // head_group]
        v_rows = value_head_rows[head // head_group]
        q_blocks = q_heads[head].reshape(SEQUENCE_TOKENS // BLK, BLK, HEAD_SIZE)

        def one_block(item):
            q_rows, rows_pos = item
            scores = jnp.dot(q_rows, k_rows.T, preferred_element_type=jnp.float32) * scale
            visible = positions[None, :] <= rows_pos[:, None]
            top = lax.optimization_barrier(jnp.max(jnp.where(visible, scores, -jnp.inf), axis=1, keepdims=True))
            weights = jnp.where(visible, jnp.exp(scores - top), 0.0)
            total = lax.optimization_barrier(jnp.sum(weights, axis=1, keepdims=True))
            return jnp.dot(weights.astype(jnp.bfloat16), v_rows, preferred_element_type=jnp.float32) / total
        return lax.map(one_block, (q_blocks, q_pos)).reshape(SEQUENCE_TOKENS, HEAD_SIZE)
    heads_out = lax.map(one_head, jnp.arange(QUERY_HEADS, dtype=jnp.int32))
    attended = jnp.transpose(heads_out, (1, 0, 2)).reshape(SEQUENCE_TOKENS, QUERY_HEADS * HEAD_SIZE).astype(jnp.bfloat16)
    return jnp.dot(attended, out_weight, preferred_element_type=jnp.float32).astype(jnp.bfloat16)
```

```python
import functools
import math

import jax
import jax.numpy as jnp
from jax import lax
from jax.experimental import pallas as pl
from jax.experimental.pallas import tpu as pltpu
from jax.sharding import PartitionSpec as P

F32 = jnp.float32
BF = jnp.bfloat16
MESH = pl.DeviceIdType.MESH
HEAD = 128
BLK = 128
HEADS_DEV = 4
ROWS = 256
NX, NZL, NY = 4, 8, 4
LOG_SCALE = math.log2(math.e) / math.sqrt(HEAD)
LOW = -1e30
HIGH = 1e30

KROWS = BLK + 16
SLOT_ROWS = KROWS + HEAD
RIGHT = {1: 1, 2: 3, 3: 5, 4: 7}
LEFT = {1: 2, 2: 4, 3: 6}
GROUPS = [[0], [1, 2], [3, 4], [5, 6], [7]]


def beside(p):
    return [(dx, j, c) for j in GROUPS[p] for dx in (1, 2) for c in (0, 1)]


def column(p):
    return [(0, j, c) for j in GROUPS[p] for c in (0, 1)]


def across(p):
    return [(3, j, c) for j in GROUPS[p] for c in (0, 1)]


CHUNKS = [
    beside(0) + column(1),
    beside(1),
    column(2) + across(1),
    beside(2),
    column(3) + across(2),
    beside(3),
    across(3) + column(4) + across(0),
    beside(4) + across(4),
]
SLOT = {(0, 0, 0): 0, (0, 0, 1): 1}
for group in CHUNKS:
    for name in group:
        SLOT[name] = len(SLOT)
BASES = [SLOT[group[0]] for group in CHUNKS]


def kernel(
    q_hbm, k_hbm, v_hbm, w_hbm, order_ref, out_ref,
    kv, far, vtmp, vfar, q_ref, qt, s_ref, m_ref, acc, att, wbuf,
    keep, send1, recv1, send2, recv2, zsend, zpass, zrecv,
    load_sem, w_sem, send_sem, z_sem, x_sem, x2_sem, sib_sem, wx_sem, att_sem, r_sem, rs_sem,
):
    ctx = lax.axis_index("ctx")
    tp = lax.axis_index("tp")
    x, zl = ctx // NZL, ctx % NZL
    y, zh, core = tp // 4, (tp // 2) % 2, tp % 2
    zo = 1 - zh
    head = tp // 2
    far_head = y * 2 + zo

    def device(x_=None, zl_=None, y_=None, zh_=None, core_=None):
        x_ = x if x_ is None else x_
        zl_ = zl if zl_ is None else zl_
        y_ = y if y_ is None else y_
        zh_ = zh if zh_ is None else zh_
        core_ = core if core_ is None else core_
        return {"ctx": x_ * NZL + zl_, "tp": y_ * 4 + zh_ * 2 + core_}

    def along_z(step):
        z = (zh * NZL + zl + step + 2 * NZL) % (2 * NZL)
        return device(zl_=z % NZL, zh_=z // NZL)

    sibling = device(core_=1 - core)
    x_up, x_down = device(x_=(x + 1) % NX), device(x_=(x + NX - 1) % NX)
    y_near = y + 1 - 2 * (y % 2)
    y_wrap = NY - 1 - y
    y_diag = (y + 2) % NY
    y1, y2 = device(y_=y_near), device(y_=y_wrap)

    barrier = pltpu.get_barrier_semaphore()
    friends = [sibling, x_up, x_down, y1, y2] + [along_z(s) for s in (1, -1, 2, -2, 3, -3, 4, -4)]
    for friend in friends:
        pl.semaphore_signal(barrier, inc=1, device_id=friend, device_id_type=MESH)

    mine = pl.ds(pl.multiple_of(core * BLK, BLK), BLK)
    other = pl.ds(pl.multiple_of((1 - core) * BLK, BLK), BLK)
    own_cols = pl.ds(pl.multiple_of(head * HEAD, HEAD), HEAD)
    far_cols = pl.ds(pl.multiple_of(far_head * HEAD, HEAD), HEAD)
    loads = [
        pltpu.make_async_copy(v_hbm.at[mine, own_cols], vtmp.at[0], load_sem.at[0]),
        pltpu.make_async_copy(v_hbm.at[mine, far_cols], vfar, load_sem.at[1]),
        pltpu.make_async_copy(v_hbm.at[other, own_cols], vtmp.at[1], load_sem.at[2]),
        pltpu.make_async_copy(k_hbm.at[mine, own_cols], kv.at[0, 0:BLK], load_sem.at[3]),
        pltpu.make_async_copy(k_hbm.at[other, own_cols], kv.at[1, 0:BLK], load_sem.at[4]),
        pltpu.make_async_copy(k_hbm.at[mine, far_cols], far.at[0:BLK], load_sem.at[5]),
        pltpu.make_async_copy(q_hbm, q_ref, load_sem.at[6]),
    ]
    for load in loads:
        load.start()

    def w_cols(q, core_):
        return pl.ds(pl.multiple_of((q * 2 + core_) * ROWS, ROWS), ROWS)

    w_loads = [
        pltpu.make_async_copy(w_hbm.at[:, w_cols(q, core)], wbuf.at[q, 0:512], w_sem.at[q]) for q in range(8)
    ]
    place = [order_ref[0].astype(F32), order_ref[1].astype(F32)]
    my_place = order_ref[core].astype(F32)
    other_place = order_ref[1 - core].astype(F32)

    def transposed(v):
        return jnp.transpose(v.astype(F32)).astype(BF)

    kv[0, BLK:KROWS] = jnp.full((16, HEAD), my_place, F32).astype(BF)
    kv[1, BLK:KROWS] = jnp.full((16, HEAD), other_place, F32).astype(BF)
    far[BLK:KROWS] = jnp.full((16, HEAD), my_place, F32).astype(BF)
    loads[0].wait()
    kv[0, KROWS:SLOT_ROWS] = transposed(vtmp[0])
    loads[1].wait()
    far[KROWS:SLOT_ROWS] = transposed(vfar[...])
    loads[2].wait()
    kv[1, KROWS:SLOT_ROWS] = transposed(vtmp[1])
    for load in loads[3:]:
        load.wait()
    for load in w_loads:
        load.start()
    pl.semaphore_wait(barrier, len(friends))

    pending = []
    counter = [0]

    def send(src, dst, recv, target, when=None):
        copy = pltpu.make_async_remote_copy(
            src_ref=src, dst_ref=dst, send_sem=send_sem.at[counter[0]], recv_sem=recv,
            device_id=target, device_id_type=MESH,
        )
        counter[0] += 1
        pending.append((copy, when))
        if when is None:
            copy.start()
        else:
            pl.when(when)(copy.start)

    def arrived(dst, recv):
        pltpu.make_async_remote_copy(
            src_ref=dst, dst_ref=dst, send_sem=recv, recv_sem=recv, device_id=sibling, device_id_type=MESH
        ).wait_recv()

    def slot(dx, j, c):
        return kv.at[SLOT[(dx, j, c)]]

    def spread(j):
        send(slot(0, j, 0), slot(1, j, 0), x_sem.at[0, j], x_up)
        send(slot(0, j, 0), slot(2, j, 0), x_sem.at[1, j], x_down)

    def share(dx, j):
        send(slot(dx, j, 0), slot(dx, j, 1), sib_sem.at[dx, j], sibling)

    def column_event(p):
        for j in GROUPS[p]:
            arrived(slot(0, j, 0), z_sem.at[j])
            for d in (1, 2, 3):
                if RIGHT[d] == j:
                    n = RIGHT[d + 1]
                    send(slot(0, j, 0), slot(0, n, 0), z_sem.at[n], along_z(1), zl < NZL - 1)
            for d in (1, 2):
                if LEFT[d] == j:
                    n = LEFT[d + 1]
                    send(slot(0, j, 0), slot(0, n, 0), z_sem.at[n], along_z(-1), zl > 0)
            spread(j)
            share(0, j)

    def beside_event(p):
        for j in GROUPS[p]:
            arrived(slot(1, j, 0), x_sem.at[0, j])
            send(slot(1, j, 0).at[0:KROWS], slot(3, j, 0).at[0:KROWS], x2_sem.at[0, j], x_up)
            arrived(slot(2, j, 0), x_sem.at[1, j])
            send(
                slot(2, j, 0).at[KROWS:SLOT_ROWS], slot(3, j, 0).at[KROWS:SLOT_ROWS], x2_sem.at[1, j], x_down
            )
            share(1, j)
            share(2, j)

    def across_event(p):
        for j in GROUPS[p]:
            arrived(slot(3, j, 0).at[0:KROWS], x2_sem.at[0, j])
            arrived(slot(3, j, 0).at[KROWS:SLOT_ROWS], x2_sem.at[1, j])
            share(3, j)

    def w_send(q):
        send(w_hbm.at[:, w_cols(q, 1 - core)], wbuf.at[q, 512:1024], wx_sem.at[q], sibling)

    def prepare_queries():
        for h in range(HEADS_DEV):
            t = jnp.transpose(q_ref[:, h * HEAD : (h + 1) * HEAD].astype(F32)) * LOG_SCALE
            top = t.astype(BF)
            qt[h, 0:HEAD] = top
            qt[h, HEAD : 2 * HEAD] = (t - top.astype(F32)).astype(BF)

    q_place = jnp.concatenate([jnp.full((1, BLK), place[0], F32), jnp.full((1, BLK), place[1], F32)], axis=1)

    def keys_values(base, count):
        ks, vs = [], []
        for i in range(count):
            k = kv[base + i, 0:BLK]
            ks.append(jnp.concatenate([k, k], axis=1))
            vs.append(kv[base + i, KROWS:SLOT_ROWS])
        values = jnp.concatenate([jnp.concatenate(vs, axis=1), jnp.ones((16, count * BLK), BF)], axis=0)
        return jnp.concatenate(ks, axis=0), values

    def own_chunk():
        keys, values = keys_values(0, 2)
        rows = lax.broadcasted_iota(jnp.int32, (BLK, ROWS), 0).astype(F32)
        lanes = (lax.broadcasted_iota(jnp.int32, (1, ROWS), 1) % BLK).astype(F32)
        q_pos = q_place * BLK + lanes
        seen = [rows + my_place * BLK <= q_pos, rows + other_place * BLK <= q_pos]
        for h in range(HEADS_DEV):
            s = jnp.dot(keys, qt[h], preferred_element_type=F32)
            parts = [jnp.where(seen[i], s[i * BLK : (i + 1) * BLK], LOW) for i in range(2)]
            top = jnp.maximum(
                jnp.max(parts[0], axis=0, keepdims=True), jnp.max(parts[1], axis=0, keepdims=True)
            )
            weights = jnp.concatenate([jnp.exp2(part - top).astype(BF) for part in parts], axis=0)
            acc[h] = jnp.dot(values, weights, preferred_element_type=F32)
            m_ref[h, 0:1] = top

    def chunk(n):
        base, count = BASES[n], len(CHUNKS[n])
        for dx, j, c in CHUNKS[n]:
            if c == 1:
                arrived(slot(dx, j, 1), sib_sem.at[dx, j])
        keys, values = keys_values(base, count)
        seen = []
        for i in range(count):
            p = kv[base + i, BLK:KROWS].astype(F32)[0:1]
            seen.append(jnp.concatenate([p, p], axis=1) < q_place)
        for h in range(HEADS_DEV):
            s_ref[h, 0 : count * BLK] = jnp.dot(keys, qt[h], preferred_element_type=F32)
        for h in range(HEADS_DEV):
            old = m_ref[h, 0:1]
            top = old
            for i in range(count):
                high = jnp.max(s_ref[h, i * BLK : (i + 1) * BLK], axis=0, keepdims=True)
                top = jnp.maximum(top, jnp.where(seen[i], high, LOW))
            weights = jnp.concatenate(
                [
                    jnp.exp2(s_ref[h, i * BLK : (i + 1) * BLK] - jnp.where(seen[i], top, HIGH)).astype(BF)
                    for i in range(count)
                ],
                axis=0,
            )
            acc[h] = acc[h] * jnp.exp2(old - top) + jnp.dot(values, weights, preferred_element_type=F32)
            m_ref[h, 0:1] = top

    spread(0)
    send(slot(0, 0, 0), slot(0, RIGHT[1], 0), z_sem.at[RIGHT[1]], along_z(1), zl < NZL - 1)
    send(slot(0, 0, 0), slot(0, LEFT[1], 0), z_sem.at[LEFT[1]], along_z(-1), zl > 0)
    for d in (1, 2, 3, 4):
        send(far, slot(0, RIGHT[d], 0), z_sem.at[RIGHT[d]], along_z(d), zl == NZL - d)
    for d in (1, 2, 3):
        send(far, slot(0, LEFT[d], 0), z_sem.at[LEFT[d]], along_z(-d), zl == d - 1)

    prepare_queries()
    own_chunk()
    beside_event(0)
    column_event(1)
    w_send(0)
    w_send(1)
    across_event(0)
    chunk(0)
    column_event(2)
    beside_event(1)
    chunk(1)
    across_event(1)
    w_send(2)
    w_send(3)
    chunk(2)
    column_event(3)
    beside_event(2)
    chunk(3)
    across_event(2)
    w_send(4)
    w_send(5)
    chunk(4)
    column_event(4)
    beside_event(3)
    chunk(5)
    across_event(3)
    w_send(6)
    w_send(7)
    beside_event(4)
    chunk(6)
    across_event(4)
    chunk(7)

    for h in range(HEADS_DEV):
        a = acc[h]
        att[:, h * HEAD : (h + 1) * HEAD] = jnp.transpose(a[0:HEAD] / a[HEAD : HEAD + 1]).astype(BF)
    send(att.at[:, 0:512], att.at[:, 512:1024], att_sem, sibling)
    for load in w_loads:
        load.wait()
    for q in range(8):
        arrived(wbuf.at[q, 512:1024], wx_sem.at[q])
    arrived(att.at[:, 512:1024], att_sem)

    def product(y_, zz):
        q = y_ * 2 + zz
        return jnp.dot(att[...], wbuf[q], preferred_element_type=F32)

    half = ROWS // 2
    first_to = [y1, y2]
    second_to = [y2, y1]

    def first_products(n, zz):
        d = product(y_diag, zz)
        send1[n, 0, 1] = d[0:half].astype(BF)
        send1[n, 1, 1] = d[half:ROWS].astype(BF)
        a = product(y_near, zz)
        send1[n, 0, 0] = a[0:half].astype(BF)
        keep[n, 1, 1] = a[half:ROWS]
        b = product(y_wrap, zz)
        send1[n, 1, 0] = b[half:ROWS].astype(BF)
        keep[n, 0, 1] = b[0:half]
        c = product(y, zz)
        keep[n, 0, 0] = c[0:half]
        keep[n, 1, 0] = c[half:ROWS]

    def first_sends(n):
        for f in range(2):
            send(send1.at[n, f], recv1.at[n, f], r_sem.at[0, n, f], first_to[f])

    def second_sends(n):
        for f in range(2):
            arrived(recv1.at[n, f], r_sem.at[0, n, f])
            send2[n, f] = (keep[n, f, 1] + recv1[n, f, 1].astype(F32)).astype(BF)
            send(send2.at[n, f], recv2.at[n, f], r_sem.at[1, n, f], second_to[f])

    def column_sum(n, f):
        arrived(recv2.at[n, f], r_sem.at[1, n, f])
        return keep[n, f, 0] + recv1[n, f, 0].astype(F32) + recv2[n, f].astype(F32)

    z_four = [along_z(4), along_z(-4)]
    first_products(0, zo)
    first_sends(0)
    first_products(1, zh)
    second_sends(0)
    first_sends(1)
    for f in range(2):
        zsend[f] = column_sum(0, f).astype(BF)
        send(zsend.at[f], zpass.at[f], rs_sem.at[0, f], z_four[f])
    second_sends(1)
    for f in range(2):
        arrived(zpass.at[f], rs_sem.at[0, f])
        send(zpass.at[f], zrecv.at[f], rs_sem.at[1, f], z_four[f])
    for f in range(2):
        keep[1, f, 0] = column_sum(1, f)
    for f in range(2):
        arrived(zrecv.at[f], rs_sem.at[1, f])
        out_ref[f * half : (f + 1) * half] = (keep[1, f, 0] + zrecv[f].astype(F32)).astype(BF)

    for copy, when in pending:
        if when is None:
            copy.wait_send()
        else:
            pl.when(when)(copy.wait_send)


SENDS = 192


def shards(queries, keys, values, out_weight, block_order):
    any_spec = pl.BlockSpec(memory_space=pl.ANY)
    half = ROWS // 2
    dma = pltpu.SemaphoreType.DMA
    return pl.pallas_call(
        kernel,
        out_shape=jax.ShapeDtypeStruct((ROWS, ROWS), BF),
        in_specs=[any_spec] * 4 + [pl.BlockSpec(memory_space=pltpu.SMEM)],
        out_specs=pl.BlockSpec(memory_space=pltpu.VMEM),
        scratch_shapes=[
            pltpu.VMEM((64, SLOT_ROWS, HEAD), BF),
            pltpu.VMEM((SLOT_ROWS, HEAD), BF),
            pltpu.VMEM((2, BLK, HEAD), BF),
            pltpu.VMEM((BLK, HEAD), BF),
            pltpu.VMEM((ROWS, HEADS_DEV * HEAD), BF),
            pltpu.VMEM((HEADS_DEV, 2 * HEAD, ROWS), BF),
            pltpu.VMEM((HEADS_DEV, 8 * BLK, ROWS), F32),
            pltpu.VMEM((HEADS_DEV, 8, ROWS), F32),
            pltpu.VMEM((HEADS_DEV, HEAD + 16, ROWS), F32),
            pltpu.VMEM((ROWS, 1024), BF),
            pltpu.VMEM((8, 1024, ROWS), BF),
            pltpu.VMEM((2, 2, 2, half, ROWS), F32),
            pltpu.VMEM((2, 2, 2, half, ROWS), BF),
            pltpu.VMEM((2, 2, 2, half, ROWS), BF),
            pltpu.VMEM((2, 2, half, ROWS), BF),
            pltpu.VMEM((2, 2, half, ROWS), BF),
            pltpu.VMEM((2, half, ROWS), BF),
            pltpu.VMEM((2, half, ROWS), BF),
            pltpu.VMEM((2, half, ROWS), BF),
            dma((7,)),
            dma((8,)),
            dma((SENDS,)),
            dma((8,)),
            dma((2, 8)),
            dma((2, 8)),
            dma((4, 8)),
            dma((8,)),
            dma,
            dma((2, 2, 2)),
            dma((2, 2)),
        ],
        compiler_params=pltpu.CompilerParams(
            collective_id=0, has_side_effects=True, vmem_limit_bytes=56 * 2**20
        ),
    )(queries, keys, values, out_weight, block_order)


def solution(mesh):
    in_specs = (P("ctx", "tp"), P("ctx", None), P("ctx", None), P("tp", None), P("ctx"))
    out_specs = P("ctx", "tp")
    return jax.shard_map(shards, mesh=mesh, in_specs=in_specs, out_specs=out_specs, check_vma=False)
```

```python
import functools
import math

import jax
import jax.numpy as jnp
from jax import lax
from jax.experimental import pallas as pl
from jax.experimental.pallas import tpu as pltpu
from jax.sharding import PartitionSpec as P

F32 = jnp.float32
BF = jnp.bfloat16
MESH = pl.DeviceIdType.MESH
HEAD = 128
BLK = 128
HEADS_DEV = 4
ROWS = 256
NX, NZL, NY = 4, 8, 4
LOG_SCALE = math.log2(math.e) / math.sqrt(HEAD)
LOW = -1e30
HIGH = 1e30

KROWS = BLK + 16
SLOT_ROWS = KROWS + HEAD
GROUPS = [[0], [1, 2], [3, 4], [5, 6], [7]]


def group(kind, p):
    side = (1, 2) if kind == "beside" else (0,) if kind == "column" else (3,)
    return [(dx, j, c) for c in (0, 1) for j in GROUPS[p] for dx in side]


CHUNKS = [
    [("beside", 0), ("column", 1)],
    [("beside", 1)],
    [("column", 2), ("across", 1)],
    [("beside", 2)],
    [("column", 3), ("across", 2)],
    [("beside", 3)],
    [("across", 3), ("column", 4), ("across", 0)],
    [("beside", 4), ("across", 4)],
]
SLOT = {(0, 0, 0): 1, (0, 0, 1): 2}
SPANS = []
for parts in CHUNKS:
    first = len(SLOT) + 1
    for part in parts:
        for name in group(*part):
            SLOT[name] = len(SLOT) + 1
    SPANS.append((first, len(SLOT) + 1 - first))
SLOTS = len(SLOT) + 1


def kernel(
    q_hbm, k_hbm, v_hbm, w_hbm, order_ref, out_ref,
    kv, vtmp, q_ref, qt, s_ref, m_ref, acc, att, wbuf,
    keep, send1, recv1, send2, recv2, zsend, zrecv,
    load_sem, w_sem, send_sem, z_sem, x_sem, x2_sem, sib_sem, wx_sem, att_sem, att_sent, r_sem, r_sent, z8_sem, z8_sent,
):
    ctx = lax.axis_index("ctx")
    tp = lax.axis_index("tp")
    x, zl = ctx // NZL, ctx % NZL
    y, zh, core = tp // 4, (tp // 2) % 2, tp % 2
    zo = 1 - zh
    head = tp // 2
    far_head = y * 2 + zo

    def device(x_=None, zl_=None, y_=None, zh_=None, core_=None):
        x_ = x if x_ is None else x_
        zl_ = zl if zl_ is None else zl_
        y_ = y if y_ is None else y_
        zh_ = zh if zh_ is None else zh_
        core_ = core if core_ is None else core_
        return {"ctx": x_ * NZL + zl_, "tp": y_ * 4 + zh_ * 2 + core_}

    def along_z(step):
        z = (zh * NZL + zl + step + 2 * NZL) % (2 * NZL)
        return device(zl_=z % NZL, zh_=z // NZL)

    sibling = device(core_=1 - core)
    x_over, z_over = device(x_=(x + 2) % NX), device(zh_=zo)
    x_up, x_down = device(x_=(x + 1) % NX), device(x_=(x + NX - 1) % NX)
    y_near = y + 1 - 2 * (y % 2)
    y_wrap = NY - 1 - y
    y_diag = (y + 2) % NY
    y1, y2 = device(y_=y_near), device(y_=y_wrap)

    barrier = pltpu.get_barrier_semaphore()
    friends = [sibling, x_up, x_down, x_over, y1, y2, z_over]
    friends += [along_z(s) for s in (1, -1, 2, -2, 3, -3, 4, -4)]
    for friend in friends:
        pl.semaphore_signal(barrier, inc=1, device_id=friend, device_id_type=MESH)

    mine = pl.ds(pl.multiple_of(core * BLK, BLK), BLK)
    other = pl.ds(pl.multiple_of((1 - core) * BLK, BLK), BLK)
    own_cols = pl.ds(pl.multiple_of(head * HEAD, HEAD), HEAD)
    far_cols = pl.ds(pl.multiple_of(far_head * HEAD, HEAD), HEAD)
    loads = [
        pltpu.make_async_copy(v_hbm.at[mine, own_cols], vtmp.at[0], load_sem.at[0]),
        pltpu.make_async_copy(v_hbm.at[mine, far_cols], vtmp.at[1], load_sem.at[1]),
        pltpu.make_async_copy(v_hbm.at[other, own_cols], vtmp.at[2], load_sem.at[2]),
        pltpu.make_async_copy(k_hbm.at[mine, own_cols], kv.at[1, 0:BLK], load_sem.at[3]),
        pltpu.make_async_copy(k_hbm.at[mine, far_cols], kv.at[0, 0:BLK], load_sem.at[4]),
        pltpu.make_async_copy(k_hbm.at[other, own_cols], kv.at[2, 0:BLK], load_sem.at[5]),
        pltpu.make_async_copy(q_hbm, q_ref, load_sem.at[6]),
    ]
    for load in loads:
        load.start()

    def w_cols(q, core_):
        return pl.ds(pl.multiple_of((q * 2 + core_) * ROWS, ROWS), ROWS)

    def w_loaded():
        whole = wbuf.at[:, 0:512]
        return pltpu.make_async_copy(whole, whole, w_sem)

    place = [order_ref[0].astype(F32), order_ref[1].astype(F32)]
    my_place = order_ref[core].astype(F32)
    other_place = order_ref[1 - core].astype(F32)

    def transposed(v):
        return jnp.transpose(v.astype(F32)).astype(BF)

    for i, (which, load) in enumerate([(my_place, 1), (my_place, 0), (other_place, 2)]):
        kv[load, BLK:KROWS] = jnp.full((16, HEAD), which, F32).astype(BF)
        loads[i].wait()
        kv[load, KROWS:SLOT_ROWS] = transposed(vtmp[i])
    for load in loads[3:]:
        load.wait()
    for q in range(8):
        pltpu.make_async_copy(w_hbm.at[:, w_cols(q, core)], wbuf.at[q, 0:512], w_sem).start()
    pl.semaphore_wait(barrier, len(friends))

    def send(src, dst, recv, target, sent=None):
        pltpu.make_async_remote_copy(
            src_ref=src, dst_ref=dst, send_sem=send_sem if sent is None else sent, recv_sem=recv,
            device_id=target, device_id_type=MESH,
        ).start()

    def landed(ref, sem):
        return pltpu.make_async_remote_copy(
            src_ref=ref, dst_ref=ref, send_sem=sem, recv_sem=sem, device_id=sibling, device_id_type=MESH
        )

    def arrived(ref, sem):
        landed(ref, sem).wait_recv()

    def slot(dx, j, c):
        return kv.at[SLOT[(dx, j, c)]]

    def part(kind, p, c):
        names = group(kind, p)
        count = len(names) // 2
        return kv.at[pl.ds(SLOT[names[c * count]], count)]

    KINDS = {"column": 0, "beside": 1, "across": 2}

    def spread(p, j):
        send(slot(0, j, 0), slot(1, j, 0), x_sem.at[p], x_up)
        send(slot(0, j, 0), slot(2, j, 0), x_sem.at[p], x_down)
        send(slot(0, j, 0), slot(3, j, 0), x2_sem.at[p], x_over)

    def share(kind, p):
        send(part(kind, p, 0), part(kind, p, 1), sib_sem.at[KINDS[kind], p], sibling)

    def column_event(p):
        for j in GROUPS[p]:
            arrived(slot(0, j, 0), z_sem.at[j])
            spread(p, j)
        share("column", p)

    def beside_event(p):
        arrived(part("beside", p, 0), x_sem.at[p])
        share("beside", p)

    def across_event(p):
        arrived(part("across", p, 0), x2_sem.at[p])
        share("across", p)

    def w_send(q):
        send(w_hbm.at[:, w_cols(q, 1 - core)], wbuf.at[q, 512:1024], wx_sem.at[0], sibling, wx_sem.at[1])

    def prepare_queries():
        for h in range(HEADS_DEV):
            t = jnp.transpose(q_ref[:, h * HEAD : (h + 1) * HEAD].astype(F32)) * LOG_SCALE
            top = t.astype(BF)
            qt[h, 0:HEAD] = top
            qt[h, HEAD : 2 * HEAD] = (t - top.astype(F32)).astype(BF)

    q_place = jnp.concatenate([jnp.full((1, BLK), place[0], F32), jnp.full((1, BLK), place[1], F32)], axis=1)

    def keys_values(base, count):
        ks, vs = [], []
        for i in range(count):
            k = kv[base + i, 0:BLK]
            ks.append(jnp.concatenate([k, k], axis=1))
            vs.append(kv[base + i, KROWS:SLOT_ROWS])
        values = jnp.concatenate([jnp.concatenate(vs, axis=1), jnp.ones((16, count * BLK), BF)], axis=0)
        return jnp.concatenate(ks, axis=0), values

    def own_chunk():
        keys, values = keys_values(1, 2)
        rows = lax.broadcasted_iota(jnp.int32, (BLK, ROWS), 0).astype(F32)
        lanes = (lax.broadcasted_iota(jnp.int32, (1, ROWS), 1) % BLK).astype(F32)
        q_pos = q_place * BLK + lanes
        seen = [rows + my_place * BLK <= q_pos, rows + other_place * BLK <= q_pos]
        for h in range(HEADS_DEV):
            s = jnp.dot(keys, qt[h], preferred_element_type=F32)
            parts = [jnp.where(seen[i], s[i * BLK : (i + 1) * BLK], LOW) for i in range(2)]
            top = jnp.maximum(
                jnp.max(parts[0], axis=0, keepdims=True), jnp.max(parts[1], axis=0, keepdims=True)
            )
            weights = jnp.concatenate([jnp.exp2(part - top).astype(BF) for part in parts], axis=0)
            acc[h] = jnp.dot(values, weights, preferred_element_type=F32)
            m_ref[h, 0:1] = top

    def chunk(n):
        base, count = SPANS[n]
        for kind, p in CHUNKS[n]:
            arrived(part(kind, p, 1), sib_sem.at[KINDS[kind], p])
        keys, values = keys_values(base, count)
        seen = []
        for i in range(count):
            p = kv[base + i, BLK:KROWS].astype(F32)[0:1]
            seen.append(jnp.concatenate([p, p], axis=1) < q_place)
        for h in range(HEADS_DEV):
            s_ref[h, 0 : count * BLK] = jnp.dot(keys, qt[h], preferred_element_type=F32)
        for h in range(HEADS_DEV):
            old = m_ref[h, 0:1]
            top = old
            for i in range(count):
                high = jnp.max(s_ref[h, i * BLK : (i + 1) * BLK], axis=0, keepdims=True)
                top = jnp.maximum(top, jnp.where(seen[i], high, LOW))
            weights = jnp.concatenate(
                [
                    jnp.exp2(s_ref[h, i * BLK : (i + 1) * BLK] - jnp.where(seen[i], top, HIGH)).astype(BF)
                    for i in range(count)
                ],
                axis=0,
            )
            acc[h] = acc[h] * jnp.exp2(old - top) + jnp.dot(values, weights, preferred_element_type=F32)
            m_ref[h, 0:1] = top

    def for_step(step):
        return kv.at[jnp.where((zl + step >= 0) & (zl + step < NZL), 1, 0)]

    def right(d):
        j = 2 * d - 1
        send(for_step(d), slot(0, j, 0), z_sem.at[j], along_z(d))

    def left(d):
        j = 2 * d
        send(for_step(-d), slot(0, j, 0), z_sem.at[j], along_z(-d))

    right(1)
    left(1)
    spread(0, 0)
    right(2)
    left(2)
    right(3)
    left(3)
    send(for_step(4).at[0:KROWS], slot(0, 7, 0).at[0:KROWS], z_sem.at[7], along_z(4))
    send(for_step(-4).at[KROWS:SLOT_ROWS], slot(0, 7, 0).at[KROWS:SLOT_ROWS], z_sem.at[7], along_z(-4))

    prepare_queries()
    own_chunk()
    column_event(1)
    beside_event(0)
    across_event(0)
    w_send(0)
    w_send(1)
    chunk(0)
    column_event(2)
    beside_event(1)
    w_send(2)
    w_send(3)
    chunk(1)
    column_event(3)
    across_event(1)
    w_send(4)
    w_send(5)
    chunk(2)
    column_event(4)
    beside_event(2)
    w_send(6)
    w_send(7)
    chunk(3)
    across_event(2)
    chunk(4)
    beside_event(3)
    chunk(5)
    across_event(3)
    chunk(6)
    beside_event(4)
    across_event(4)
    chunk(7)

    for h in range(HEADS_DEV):
        a = acc[h]
        att[:, h * HEAD : (h + 1) * HEAD] = jnp.transpose(a[0:HEAD] / a[HEAD : HEAD + 1]).astype(BF)
    send(att.at[:, 0:512], att.at[:, 512:1024], att_sem, sibling, att_sent)
    w_loaded().wait()
    arrived(wbuf.at[:, 512:1024], wx_sem.at[0])
    arrived(att.at[:, 512:1024], att_sem)

    def product(y_, zz):
        q = y_ * 2 + zz
        return jnp.dot(att[...], wbuf[q], preferred_element_type=F32)

    half = ROWS // 2
    first_to = [y1, y2]
    second_to = [y2, y1]

    def first_products(n, zz):
        d = product(y_diag, zz)
        send1[n, 0, 1] = d[0:half].astype(BF)
        send1[n, 1, 1] = d[half:ROWS].astype(BF)
        a = product(y_near, zz)
        send1[n, 0, 0] = a[0:half].astype(BF)
        keep[n, 1, 1] = a[half:ROWS]
        b = product(y_wrap, zz)
        send1[n, 1, 0] = b[half:ROWS].astype(BF)
        keep[n, 0, 1] = b[0:half]
        c = product(y, zz)
        keep[n, 0, 0] = c[0:half]
        keep[n, 1, 0] = c[half:ROWS]

    piece = half // 2

    def rows(u):
        return pl.ds(u * piece, piece)

    def first_send(n, f, u):
        send(
            send1.at[n, f, :, rows(u)], recv1.at[n, f, :, rows(u)], r_sem.at[0, n, f, u], first_to[f], r_sent.at[0]
        )

    def second_send(n, f, u):
        arrived(recv1.at[n, f, :, rows(u)], r_sem.at[0, n, f, u])
        send2[n, f, rows(u)] = (keep[n, f, 1, rows(u)] + recv1[n, f, 1, rows(u)].astype(F32)).astype(BF)
        send(send2.at[n, f, rows(u)], recv2.at[n, f, rows(u)], r_sem.at[1, n, f, u], second_to[f], r_sent.at[1])

    def column_sum(n, f, u):
        arrived(recv2.at[n, f, rows(u)], r_sem.at[1, n, f, u])
        return keep[n, f, 0, rows(u)] + recv1[n, f, 0, rows(u)].astype(F32) + recv2[n, f, rows(u)].astype(F32)

    steps = [(f, u) for u in range(2) for f in range(2)]
    first_products(0, zo)
    for f, u in steps:
        first_send(0, f, u)
    first_products(1, zh)
    for f, u in steps:
        second_send(0, f, u)
    for f, u in steps:
        first_send(1, f, u)
    for f, u in steps:
        zsend[f, rows(u)] = column_sum(0, f, u).astype(BF)
        send(zsend.at[f, rows(u)], zrecv.at[f, rows(u)], z8_sem.at[f, u], z_over, z8_sent)
    for f, u in steps:
        second_send(1, f, u)
    for f, u in steps:
        keep[1, f, 0, rows(u)] = column_sum(1, f, u)
    for f, u in steps:
        arrived(zrecv.at[f, rows(u)], z8_sem.at[f, u])
        out_ref[pl.ds(f * half + u * piece, piece)] = (
            keep[1, f, 0, rows(u)] + zrecv[f, rows(u)].astype(F32)
        ).astype(BF)

    landed(kv.at[pl.ds(0, 62)], send_sem).wait_send()
    landed(wbuf.at[:, 512:1024], wx_sem.at[1]).wait_send()
    landed(att.at[:, 0:512], att_sent).wait_send()
    landed(send1, r_sent.at[0]).wait_send()
    landed(send2, r_sent.at[1]).wait_send()
    landed(zsend, z8_sent).wait_send()


def shards(queries, keys, values, out_weight, block_order):
    any_spec = pl.BlockSpec(memory_space=pl.ANY)
    half = ROWS // 2
    dma = pltpu.SemaphoreType.DMA
    return pl.pallas_call(
        kernel,
        out_shape=jax.ShapeDtypeStruct((ROWS, ROWS), BF),
        in_specs=[any_spec] * 4 + [pl.BlockSpec(memory_space=pltpu.SMEM)],
        out_specs=pl.BlockSpec(memory_space=pltpu.VMEM),
        scratch_shapes=[
            pltpu.VMEM((SLOTS, SLOT_ROWS, HEAD), BF),
            pltpu.VMEM((3, BLK, HEAD), BF),
            pltpu.VMEM((ROWS, HEADS_DEV * HEAD), BF),
            pltpu.VMEM((HEADS_DEV, 2 * HEAD, ROWS), BF),
            pltpu.VMEM((HEADS_DEV, 8 * BLK, ROWS), F32),
            pltpu.VMEM((HEADS_DEV, 8, ROWS), F32),
            pltpu.VMEM((HEADS_DEV, HEAD + 16, ROWS), F32),
            pltpu.VMEM((ROWS, 1024), BF),
            pltpu.VMEM((8, 1024, ROWS), BF),
            pltpu.VMEM((2, 2, 2, half, ROWS), F32),
            pltpu.VMEM((2, 2, 2, half, ROWS), BF),
            pltpu.VMEM((2, 2, 2, half, ROWS), BF),
            pltpu.VMEM((2, 2, half, ROWS), BF),
            pltpu.VMEM((2, 2, half, ROWS), BF),
            pltpu.VMEM((2, half, ROWS), BF),
            pltpu.VMEM((2, half, ROWS), BF),
            dma((7,)),
            dma,
            dma,
            dma((8,)),
            dma((5,)),
            dma((5,)),
            dma((3, 5)),
            dma((2,)),
            dma,
            dma,
            dma((2, 2, 2, 2)),
            dma((2,)),
            dma((2, 2)),
            dma,
        ],
        compiler_params=pltpu.CompilerParams(
            collective_id=0, has_side_effects=True, vmem_limit_bytes=56 * 2**20
        ),
    )(queries, keys, values, out_weight, block_order)


def solution(mesh):
    in_specs = (P("ctx", "tp"), P("ctx", None), P("ctx", None), P("tp", None), P("ctx"))
    out_specs = P("ctx", "tp")
    return jax.shard_map(shards, mesh=mesh, in_specs=in_specs, out_specs=out_specs, check_vma=False)
```

```python
import functools
import math

import jax
import jax.numpy as jnp
from jax import lax
from jax.experimental import pallas as pl
from jax.experimental.pallas import tpu as pltpu
from jax.sharding import PartitionSpec as P

F32 = jnp.float32
BF = jnp.bfloat16
MESH = pl.DeviceIdType.MESH
HEAD = 128
BLK = 128
HEADS_DEV = 4
ROWS = 256
NX, NZL, NY = 4, 8, 4
LOG_SCALE = math.log2(math.e) / math.sqrt(HEAD)
LOW = -1e30
HIGH = 1e30

KROWS = BLK + 16
SLOT_ROWS = KROWS + HEAD
GROUPS = [[0], [1, 2], [3, 4], [5, 6], [7]]


def group(kind, p):
    side = (1, 2) if kind == "beside" else (0,) if kind == "column" else (3,)
    return [(dx, j, c) for c in (0, 1) for j in GROUPS[p] for dx in side]


CHUNKS = [
    [("beside", 0), ("column", 1)],
    [("beside", 1)],
    [("across", 0), ("column", 2)],
    [("beside", 2)],
    [("across", 1), ("column", 3)],
    [("beside", 3)],
    [("across", 2), ("column", 4)],
    [("beside", 4), ("across", 3)],
    [("across", 4)],
]
SLOT = {(0, 0, 0): 1, (0, 0, 1): 2}
SPANS = []
for parts in CHUNKS:
    first = len(SLOT) + 1
    for part in parts:
        for name in group(*part):
            SLOT[name] = len(SLOT) + 1
    SPANS.append((first, len(SLOT) + 1 - first))
SLOTS = len(SLOT) + 1
PIECES = 4
LATE = 3
RELAYED = (0, 1, 2, 3)


def kernel(
    q_hbm, k_hbm, v_hbm, w_hbm, order_ref, out_ref,
    kv, vtmp, q_ref, qt, s_ref, m_ref, acc, att, wbuf,
    keep, send1, recv1, zsend, zrecv,
    load_sem, w_sem, send_sem, z_sem, x_sem, x2_sem, sib_sem, wx_sem, att_sem, att_sent, r_sem, r_sent, z8_sem, z8_sent,
):
    ctx = lax.axis_index("ctx")
    tp = lax.axis_index("tp")
    x, zl = ctx // NZL, ctx % NZL
    y, zh, core = tp // 4, (tp // 2) % 2, tp % 2
    zo = 1 - zh
    head = tp // 2
    far_head = y * 2 + zo

    def device(x_=None, zl_=None, y_=None, zh_=None, core_=None):
        x_ = x if x_ is None else x_
        zl_ = zl if zl_ is None else zl_
        y_ = y if y_ is None else y_
        zh_ = zh if zh_ is None else zh_
        core_ = core if core_ is None else core_
        return {"ctx": x_ * NZL + zl_, "tp": y_ * 4 + zh_ * 2 + core_}

    def along_z(step):
        z = (zh * NZL + zl + step + 2 * NZL) % (2 * NZL)
        return device(zl_=z % NZL, zh_=z // NZL)

    sibling = device(core_=1 - core)
    x_over, z_over = device(x_=(x + 2) % NX), device(zh_=zo)
    x_up, x_down = device(x_=(x + 1) % NX), device(x_=(x + NX - 1) % NX)
    y_near = y + 1 - 2 * (y % 2)
    y_wrap = NY - 1 - y
    y_diag = (y + 2) % NY
    y1, y2, y_over = device(y_=y_near), device(y_=y_wrap), device(y_=y_diag)

    barrier = pltpu.get_barrier_semaphore()
    friends = [sibling, x_up, x_down, x_over, y1, y2, y_over]
    friends += [along_z(s) for s in (1, -1, 2, -2, 3, -3, 4, -4)]
    for friend in friends:
        pl.semaphore_signal(barrier, inc=1, device_id=friend, device_id_type=MESH)

    mine = pl.ds(pl.multiple_of(core * BLK, BLK), BLK)
    other = pl.ds(pl.multiple_of((1 - core) * BLK, BLK), BLK)
    own_cols = pl.ds(pl.multiple_of(head * HEAD, HEAD), HEAD)
    far_cols = pl.ds(pl.multiple_of(far_head * HEAD, HEAD), HEAD)
    loads = [
        pltpu.make_async_copy(v_hbm.at[mine, own_cols], vtmp.at[0], load_sem.at[0]),
        pltpu.make_async_copy(v_hbm.at[mine, far_cols], vtmp.at[1], load_sem.at[1]),
        pltpu.make_async_copy(v_hbm.at[other, own_cols], vtmp.at[2], load_sem.at[2]),
        pltpu.make_async_copy(k_hbm.at[mine, own_cols], kv.at[1, 0:BLK], load_sem.at[3]),
        pltpu.make_async_copy(k_hbm.at[mine, far_cols], kv.at[0, 0:BLK], load_sem.at[4]),
        pltpu.make_async_copy(k_hbm.at[other, own_cols], kv.at[2, 0:BLK], load_sem.at[5]),
        pltpu.make_async_copy(q_hbm, q_ref, load_sem.at[6]),
    ]
    for load in loads:
        load.start()

    def w_cols(q, core_):
        return pl.ds(pl.multiple_of((q * 2 + core_) * ROWS, ROWS), ROWS)

    def w_loaded():
        whole = wbuf.at[:, 0:512]
        return pltpu.make_async_copy(whole, whole, w_sem)

    place = [order_ref[0].astype(F32), order_ref[1].astype(F32)]
    my_place = order_ref[core].astype(F32)
    other_place = order_ref[1 - core].astype(F32)

    def transposed(v):
        return jnp.transpose(v.astype(F32)).astype(BF)

    for i, (which, load) in enumerate([(my_place, 1), (my_place, 0), (other_place, 2)]):
        kv[load, BLK:KROWS] = jnp.full((16, HEAD), which, F32).astype(BF)
        loads[i].wait()
        kv[load, KROWS:SLOT_ROWS] = transposed(vtmp[i])
    for load in loads[3:]:
        load.wait()
    for q in range(8):
        pltpu.make_async_copy(w_hbm.at[:, w_cols(q, core)], wbuf.at[q, 0:512], w_sem).start()
    pl.semaphore_wait(barrier, len(friends))

    def send(src, dst, recv, target, sent=None):
        pltpu.make_async_remote_copy(
            src_ref=src, dst_ref=dst, send_sem=send_sem if sent is None else sent, recv_sem=recv,
            device_id=target, device_id_type=MESH,
        ).start()

    def landed(ref, sem):
        return pltpu.make_async_remote_copy(
            src_ref=ref, dst_ref=ref, send_sem=sem, recv_sem=sem, device_id=sibling, device_id_type=MESH
        )

    def arrived(ref, sem):
        landed(ref, sem).wait_recv()

    def slot(dx, j, c):
        return kv.at[SLOT[(dx, j, c)]]

    def part(kind, p, c):
        names = group(kind, p)
        count = len(names) // 2
        return kv.at[pl.ds(SLOT[names[c * count]], count)]

    KINDS = {"column": 0, "beside": 1, "across": 2}

    def spread(p, j):
        send(slot(0, j, 0), slot(1, j, 0), x_sem.at[p], x_up)
        send(slot(0, j, 0), slot(2, j, 0), x_sem.at[p], x_down)
        if p not in RELAYED:
            send(slot(0, j, 0), slot(3, j, 0), x2_sem.at[p], x_over)

    def share(kind, p):
        send(part(kind, p, 0), part(kind, p, 1), sib_sem.at[KINDS[kind], p], sibling)

    def column_event(p):
        for j in GROUPS[p]:
            arrived(slot(0, j, 0), z_sem.at[j])
            spread(p, j)
        share("column", p)

    def beside_event(p):
        arrived(part("beside", p, 0), x_sem.at[p])
        if p in RELAYED:
            for j in GROUPS[p]:
                keys, values = pl.ds(0, KROWS), pl.ds(KROWS, HEAD)
                send(slot(1, j, 0).at[keys], slot(3, j, 0).at[keys], x2_sem.at[p], x_up)
                send(slot(2, j, 0).at[values], slot(3, j, 0).at[values], x2_sem.at[p], x_down)
        share("beside", p)

    def across_event(p):
        arrived(part("across", p, 0), x2_sem.at[p])
        share("across", p)

    def w_send(q):
        send(w_hbm.at[:, w_cols(q, 1 - core)], wbuf.at[q, 512:1024], wx_sem.at[0], sibling, wx_sem.at[1])

    def prepare_queries():
        for h in range(HEADS_DEV):
            t = jnp.transpose(q_ref[:, h * HEAD : (h + 1) * HEAD].astype(F32)) * LOG_SCALE
            top = t.astype(BF)
            qt[h, 0:HEAD] = top
            qt[h, HEAD : 2 * HEAD] = (t - top.astype(F32)).astype(BF)

    q_place = jnp.concatenate([jnp.full((1, BLK), place[0], F32), jnp.full((1, BLK), place[1], F32)], axis=1)

    def keys_values(base, count):
        ks, vs = [], []
        for i in range(count):
            k = kv[base + i, 0:BLK]
            ks.append(jnp.concatenate([k, k], axis=1))
            vs.append(kv[base + i, KROWS:SLOT_ROWS])
        values = jnp.concatenate([jnp.concatenate(vs, axis=1), jnp.ones((16, count * BLK), BF)], axis=0)
        return jnp.concatenate(ks, axis=0), values

    def own_chunk():
        keys, values = keys_values(1, 2)
        rows = lax.broadcasted_iota(jnp.int32, (BLK, ROWS), 0).astype(F32)
        lanes = (lax.broadcasted_iota(jnp.int32, (1, ROWS), 1) % BLK).astype(F32)
        q_pos = q_place * BLK + lanes
        seen = [rows + my_place * BLK <= q_pos, rows + other_place * BLK <= q_pos]
        for h in range(HEADS_DEV):
            s = jnp.dot(keys, qt[h], preferred_element_type=F32)
            parts = [jnp.where(seen[i], s[i * BLK : (i + 1) * BLK], LOW) for i in range(2)]
            top = jnp.maximum(
                jnp.max(parts[0], axis=0, keepdims=True), jnp.max(parts[1], axis=0, keepdims=True)
            )
            weights = jnp.concatenate([jnp.exp2(part - top).astype(BF) for part in parts], axis=0)
            acc[h] = jnp.dot(values, weights, preferred_element_type=F32)
            m_ref[h, 0:1] = top

    def chunk(n):
        base, count = SPANS[n]
        for kind, p in CHUNKS[n]:
            arrived(part(kind, p, 1), sib_sem.at[KINDS[kind], p])
        keys, values = keys_values(base, count)
        seen = []
        for i in range(count):
            p = kv[base + i, BLK:KROWS].astype(F32)[0:1]
            seen.append(jnp.concatenate([p, p], axis=1) < q_place)
        for h in range(HEADS_DEV):
            s_ref[h, 0 : count * BLK] = jnp.dot(keys, qt[h], preferred_element_type=F32)
        for h in range(HEADS_DEV):
            old = m_ref[h, 0:1]
            top = old
            for i in range(count):
                high = jnp.max(s_ref[h, i * BLK : (i + 1) * BLK], axis=0, keepdims=True)
                top = jnp.maximum(top, jnp.where(seen[i], high, LOW))
            weights = jnp.concatenate(
                [
                    jnp.exp2(s_ref[h, i * BLK : (i + 1) * BLK] - jnp.where(seen[i], top, HIGH)).astype(BF)
                    for i in range(count)
                ],
                axis=0,
            )
            acc[h] = acc[h] * jnp.exp2(old - top) + jnp.dot(values, weights, preferred_element_type=F32)
            m_ref[h, 0:1] = top

    def for_step(step):
        return kv.at[jnp.where((zl + step >= 0) & (zl + step < NZL), 1, 0)]

    def right(d):
        j = 2 * d - 1
        send(for_step(d), slot(0, j, 0), z_sem.at[j], along_z(d))

    def left(d):
        j = 2 * d
        send(for_step(-d), slot(0, j, 0), z_sem.at[j], along_z(-d))

    right(1)
    left(1)
    spread(0, 0)
    right(2)
    left(2)
    right(3)
    left(3)
    send(for_step(4).at[0:KROWS], slot(0, 7, 0).at[0:KROWS], z_sem.at[7], along_z(4))
    send(for_step(-4).at[KROWS:SLOT_ROWS], slot(0, 7, 0).at[KROWS:SLOT_ROWS], z_sem.at[7], along_z(-4))

    prepare_queries()
    own_chunk()
    column_event(1)
    beside_event(0)
    column_event(2)
    w_send(0)
    w_send(1)
    chunk(0)
    beside_event(1)
    across_event(0)
    column_event(3)
    w_send(2)
    w_send(3)
    chunk(1)
    beside_event(2)
    column_event(4)
    w_send(4)
    w_send(5)
    chunk(2)
    across_event(1)
    w_send(6)
    w_send(7)
    chunk(3)
    beside_event(3)
    chunk(4)
    across_event(2)
    beside_event(4)
    chunk(5)
    across_event(3)
    chunk(6)
    across_event(4)
    chunk(7)
    chunk(8)

    for h in range(HEADS_DEV):
        a = acc[h]
        att[:, h * HEAD : (h + 1) * HEAD] = jnp.transpose(a[0:HEAD] / a[HEAD : HEAD + 1]).astype(BF)
    send(att.at[:, 0:512], att.at[:, 512:1024], att_sem, sibling, att_sent)
    w_loaded().wait()
    arrived(wbuf.at[:, 512:1024], wx_sem.at[0])
    arrived(att.at[:, 512:1024], att_sem)

    def product(y_, zz):
        return jnp.dot(att[...], wbuf[y_ * 2 + zz], preferred_element_type=F32)

    peers = [(2, y_diag, y_over), (0, y_near, y1), (1, y_wrap, y2)]
    piece = ROWS // PIECES

    def rows(u):
        return pl.ds(u * piece, piece)

    def send_terms(n, u, cut):
        part_rows = pl.ds(u * (ROWS // cut), ROWS // cut)
        for i, _, target in peers:
            send(send1.at[n, i, part_rows], recv1.at[n, i, part_rows], r_sem.at[n, u], target, r_sent)

    for i, y_, _ in peers:
        send1[0, i] = product(y_, zo).astype(BF)
    for u in range(PIECES):
        send_terms(0, u, PIECES)
    keep[0] = product(y, zo)
    for i, y_, _ in peers:
        send1[1, i] = product(y_, zh).astype(BF)
    keep[1] = product(y, zh)

    for u in range(PIECES):
        arrived(recv1.at[0, :, rows(u)], r_sem.at[0, u])
        total = keep[0, rows(u)]
        for i in range(3):
            total = total + recv1[0, i, rows(u)].astype(F32)
        zsend[rows(u)] = total.astype(BF)
        send(zsend.at[rows(u)], zrecv.at[rows(u)], z8_sem.at[u], z_over, z8_sent)
        if u == LATE:
            send_terms(1, 0, 1)
    arrived(recv1.at[1], r_sem.at[1, 0])
    for u in range(PIECES):
        total = keep[1, rows(u)]
        for i in range(3):
            total = total + recv1[1, i, rows(u)].astype(F32)
        keep[1, rows(u)] = total
    for u in range(PIECES):
        arrived(zrecv.at[rows(u)], z8_sem.at[u])
        out_ref[rows(u)] = (keep[1, rows(u)] + zrecv[rows(u)].astype(F32)).astype(BF)

    landed(kv.at[pl.ds(0, 62)], send_sem).wait_send()
    landed(wbuf.at[:, 512:1024], wx_sem.at[1]).wait_send()
    landed(att.at[:, 0:512], att_sent).wait_send()
    landed(send1, r_sent).wait_send()
    landed(zsend, z8_sent).wait_send()


def shards(queries, keys, values, out_weight, block_order):
    any_spec = pl.BlockSpec(memory_space=pl.ANY)
    dma = pltpu.SemaphoreType.DMA
    return pl.pallas_call(
        kernel,
        out_shape=jax.ShapeDtypeStruct((ROWS, ROWS), BF),
        in_specs=[any_spec] * 4 + [pl.BlockSpec(memory_space=pltpu.SMEM)],
        out_specs=pl.BlockSpec(memory_space=pltpu.VMEM),
        scratch_shapes=[
            pltpu.VMEM((SLOTS, SLOT_ROWS, HEAD), BF),
            pltpu.VMEM((3, BLK, HEAD), BF),
            pltpu.VMEM((ROWS, HEADS_DEV * HEAD), BF),
            pltpu.VMEM((HEADS_DEV, 2 * HEAD, ROWS), BF),
            pltpu.VMEM((HEADS_DEV, 8 * BLK, ROWS), F32),
            pltpu.VMEM((HEADS_DEV, 8, ROWS), F32),
            pltpu.VMEM((HEADS_DEV, HEAD + 16, ROWS), F32),
            pltpu.VMEM((ROWS, 1024), BF),
            pltpu.VMEM((8, 1024, ROWS), BF),
            pltpu.VMEM((2, ROWS, ROWS), F32),
            pltpu.VMEM((2, 3, ROWS, ROWS), BF),
            pltpu.VMEM((2, 3, ROWS, ROWS), BF),
            pltpu.VMEM((ROWS, ROWS), BF),
            pltpu.VMEM((ROWS, ROWS), BF),
            dma((7,)),
            dma,
            dma,
            dma((8,)),
            dma((5,)),
            dma((5,)),
            dma((3, 5)),
            dma((2,)),
            dma,
            dma,
            dma((2, PIECES)),
            dma,
            dma((PIECES,)),
            dma,
        ],
        compiler_params=pltpu.CompilerParams(
            collective_id=0, has_side_effects=True, vmem_limit_bytes=56 * 2**20
        ),
    )(queries, keys, values, out_weight, block_order)


def solution(mesh):
    in_specs = (P("ctx", "tp"), P("ctx", None), P("ctx", None), P("tp", None), P("ctx"))
    out_specs = P("ctx", "tp")
    return jax.shard_map(shards, mesh=mesh, in_specs=in_specs, out_specs=out_specs, check_vma=False)
```

```python
import functools
import math

import jax
import jax.numpy as jnp
from jax import lax
from jax.experimental import pallas as pl
from jax.experimental.pallas import tpu as pltpu
from jax.sharding import PartitionSpec as P

F32 = jnp.float32
BF = jnp.bfloat16
MESH = pl.DeviceIdType.MESH
HEAD = 128
BLK = 128
HEADS_DEV = 4
ROWS = 256
NX, NZL, NY = 4, 8, 4
LOG_SCALE = math.log2(math.e) / math.sqrt(HEAD)
LOW = -1e30
HIGH = 1e30

KROWS = BLK + 16
SLOT_ROWS = KROWS + HEAD
GROUPS = [[0], [1, 2], [3, 4], [5, 6], [7]]


def group(kind, p):
    side = (1, 2) if kind == "beside" else (0,) if kind == "column" else (3,)
    return [(dx, j, c) for c in (0, 1) for j in GROUPS[p] for dx in side]


CHUNKS = [
    [("beside", 0), ("column", 1)],
    [("beside", 1)],
    [("across", 0), ("column", 2)],
    [("beside", 2)],
    [("across", 1), ("column", 3)],
    [("beside", 3)],
    [("across", 2), ("column", 4)],
    [("beside", 4), ("across", 3)],
    [("across", 4)],
]
SLOT = {(0, 0, 0): 1, (0, 0, 1): 2}
SPANS = []
for parts in CHUNKS:
    first = len(SLOT) + 1
    for part in parts:
        for name in group(*part):
            SLOT[name] = len(SLOT) + 1
    SPANS.append((first, len(SLOT) + 1 - first))
SLOTS = len(SLOT) + 1
PIECES = 4
LATE = 3
RELAYED = (0, 1, 2, 3)


def kernel(
    q_hbm, k_hbm, v_hbm, w_hbm, order_ref, out_ref,
    kv, vtmp, q_ref, qt, s_ref, m_ref, acc, att, wbuf,
    keep, send1, recv1, zsend, zrecv,
    load_sem, w_sem, send_sem, z_sem, x_sem, x2_sem, sib_sem, wx_sem, att_sem, att_sent, r_sem, r_sent, z8_sem, z8_sent,
):
    ctx = lax.axis_index("ctx")
    tp = lax.axis_index("tp")
    x, zl = ctx // NZL, ctx % NZL
    y, zh, core = tp // 4, (tp // 2) % 2, tp % 2
    zo = 1 - zh
    head = tp // 2
    far_head = y * 2 + zo

    def device(x_=None, zl_=None, y_=None, zh_=None, core_=None):
        x_ = x if x_ is None else x_
        zl_ = zl if zl_ is None else zl_
        y_ = y if y_ is None else y_
        zh_ = zh if zh_ is None else zh_
        core_ = core if core_ is None else core_
        return {"ctx": x_ * NZL + zl_, "tp": y_ * 4 + zh_ * 2 + core_}

    def along_z(step):
        z = (zh * NZL + zl + step + 2 * NZL) % (2 * NZL)
        return device(zl_=z % NZL, zh_=z // NZL)

    sibling = device(core_=1 - core)
    x_over, z_over = device(x_=(x + 2) % NX), device(zh_=zo)
    x_up, x_down = device(x_=(x + 1) % NX), device(x_=(x + NX - 1) % NX)
    y_near = y + 1 - 2 * (y % 2)
    y_wrap = NY - 1 - y
    y_diag = (y + 2) % NY
    y1, y2, y_over = device(y_=y_near), device(y_=y_wrap), device(y_=y_diag)

    barrier = pltpu.get_barrier_semaphore()
    friends = [sibling, x_up, x_down, x_over, y1, y2, y_over]
    friends += [along_z(s) for s in (1, -1, 2, -2)]
    for friend in friends:
        pl.semaphore_signal(barrier, inc=1, device_id=friend, device_id_type=MESH)

    mine = pl.ds(pl.multiple_of(core * BLK, BLK), BLK)
    other = pl.ds(pl.multiple_of((1 - core) * BLK, BLK), BLK)
    own_cols = pl.ds(pl.multiple_of(head * HEAD, HEAD), HEAD)
    far_cols = pl.ds(pl.multiple_of(far_head * HEAD, HEAD), HEAD)
    loads = [
        pltpu.make_async_copy(v_hbm.at[mine, own_cols], vtmp.at[0], load_sem.at[0]),
        pltpu.make_async_copy(v_hbm.at[mine, far_cols], vtmp.at[1], load_sem.at[1]),
        pltpu.make_async_copy(v_hbm.at[other, own_cols], vtmp.at[2], load_sem.at[2]),
        pltpu.make_async_copy(k_hbm.at[mine, own_cols], kv.at[1, 0:BLK], load_sem.at[3]),
        pltpu.make_async_copy(k_hbm.at[mine, far_cols], kv.at[0, 0:BLK], load_sem.at[4]),
        pltpu.make_async_copy(k_hbm.at[other, own_cols], kv.at[2, 0:BLK], load_sem.at[5]),
        pltpu.make_async_copy(q_hbm, q_ref, load_sem.at[6]),
    ]
    for load in loads:
        load.start()

    def w_cols(q, core_):
        return pl.ds(pl.multiple_of((q * 2 + core_) * ROWS, ROWS), ROWS)

    def w_loaded():
        whole = wbuf.at[:, 0:512]
        return pltpu.make_async_copy(whole, whole, w_sem)

    place = [order_ref[0].astype(F32), order_ref[1].astype(F32)]
    my_place = order_ref[core].astype(F32)
    other_place = order_ref[1 - core].astype(F32)

    def transposed(v):
        return jnp.transpose(v.astype(F32)).astype(BF)

    for i, (which, load) in enumerate([(my_place, 1), (my_place, 0), (other_place, 2)]):
        kv[load, BLK:KROWS] = jnp.full((16, HEAD), which, F32).astype(BF)
        loads[i].wait()
        kv[load, KROWS:SLOT_ROWS] = transposed(vtmp[i])
    for load in loads[3:]:
        load.wait()
    for q in range(8):
        pltpu.make_async_copy(w_hbm.at[:, w_cols(q, core)], wbuf.at[q, 0:512], w_sem).start()
    pl.semaphore_wait(barrier, len(friends))

    def send(src, dst, recv, target, sent=None):
        pltpu.make_async_remote_copy(
            src_ref=src, dst_ref=dst, send_sem=send_sem if sent is None else sent, recv_sem=recv,
            device_id=target, device_id_type=MESH,
        ).start()

    def landed(ref, sem):
        return pltpu.make_async_remote_copy(
            src_ref=ref, dst_ref=ref, send_sem=sem, recv_sem=sem, device_id=sibling, device_id_type=MESH
        )

    def arrived(ref, sem):
        landed(ref, sem).wait_recv()

    def slot(dx, j, c):
        return kv.at[SLOT[(dx, j, c)]]

    def part(kind, p, c):
        names = group(kind, p)
        count = len(names) // 2
        return kv.at[pl.ds(SLOT[names[c * count]], count)]

    KINDS = {"column": 0, "beside": 1, "across": 2}

    def spread(p, j):
        send(slot(0, j, 0), slot(1, j, 0), x_sem.at[p], x_up)
        send(slot(0, j, 0), slot(2, j, 0), x_sem.at[p], x_down)
        if p not in RELAYED:
            send(slot(0, j, 0), slot(3, j, 0), x2_sem.at[p], x_over)

    def share(kind, p):
        send(part(kind, p, 0), part(kind, p, 1), sib_sem.at[KINDS[kind], p], sibling)

    def column_event(p):
        for j in GROUPS[p]:
            arrived(slot(0, j, 0), z_sem.at[j])
            spread(p, j)
        share("column", p)

    def beside_event(p):
        arrived(part("beside", p, 0), x_sem.at[p])
        if p in RELAYED:
            for j in GROUPS[p]:
                keys, values = pl.ds(0, KROWS), pl.ds(KROWS, HEAD)
                send(slot(1, j, 0).at[keys], slot(3, j, 0).at[keys], x2_sem.at[p], x_up)
                send(slot(2, j, 0).at[values], slot(3, j, 0).at[values], x2_sem.at[p], x_down)
        share("beside", p)

    def across_event(p):
        arrived(part("across", p, 0), x2_sem.at[p])
        share("across", p)

    def w_send(q):
        send(w_hbm.at[:, w_cols(q, 1 - core)], wbuf.at[q, 512:1024], wx_sem.at[0], sibling, wx_sem.at[1])

    def prepare_queries():
        for h in range(HEADS_DEV):
            t = jnp.transpose(q_ref[:, h * HEAD : (h + 1) * HEAD].astype(F32)) * LOG_SCALE
            top = t.astype(BF)
            qt[h, 0:HEAD] = top
            qt[h, HEAD : 2 * HEAD] = (t - top.astype(F32)).astype(BF)

    q_place = jnp.concatenate([jnp.full((1, BLK), place[0], F32), jnp.full((1, BLK), place[1], F32)], axis=1)

    def keys_values(base, count):
        ks, vs = [], []
        for i in range(count):
            k = kv[base + i, 0:BLK]
            ks.append(jnp.concatenate([k, k], axis=1))
            vs.append(kv[base + i, KROWS:SLOT_ROWS])
        values = jnp.concatenate([jnp.concatenate(vs, axis=1), jnp.ones((16, count * BLK), BF)], axis=0)
        return jnp.concatenate(ks, axis=0), values

    def own_chunk():
        keys, values = keys_values(1, 2)
        rows = lax.broadcasted_iota(jnp.int32, (BLK, ROWS), 0).astype(F32)
        lanes = (lax.broadcasted_iota(jnp.int32, (1, ROWS), 1) % BLK).astype(F32)
        q_pos = q_place * BLK + lanes
        seen = [rows + my_place * BLK <= q_pos, rows + other_place * BLK <= q_pos]
        for h in range(HEADS_DEV):
            s = jnp.dot(keys, qt[h], preferred_element_type=F32)
            parts = [jnp.where(seen[i], s[i * BLK : (i + 1) * BLK], LOW) for i in range(2)]
            top = jnp.maximum(
                jnp.max(parts[0], axis=0, keepdims=True), jnp.max(parts[1], axis=0, keepdims=True)
            )
            weights = jnp.concatenate([jnp.exp2(part - top).astype(BF) for part in parts], axis=0)
            acc[h] = jnp.dot(values, weights, preferred_element_type=F32)
            m_ref[h, 0:1] = top

    def chunk(n):
        base, count = SPANS[n]
        for kind, p in CHUNKS[n]:
            arrived(part(kind, p, 1), sib_sem.at[KINDS[kind], p])
        keys, values = keys_values(base, count)
        seen = []
        for i in range(count):
            p = kv[base + i, BLK:KROWS].astype(F32)[0:1]
            seen.append(jnp.concatenate([p, p], axis=1) < q_place)
        for h in range(HEADS_DEV):
            s_ref[h, 0 : count * BLK] = jnp.dot(keys, qt[h], preferred_element_type=F32)
        for h in range(HEADS_DEV):
            old = m_ref[h, 0:1]
            top = old
            for i in range(count):
                high = jnp.max(s_ref[h, i * BLK : (i + 1) * BLK], axis=0, keepdims=True)
                top = jnp.maximum(top, jnp.where(seen[i], high, LOW))
            weights = jnp.concatenate(
                [
                    jnp.exp2(s_ref[h, i * BLK : (i + 1) * BLK] - jnp.where(seen[i], top, HIGH)).astype(BF)
                    for i in range(count)
                ],
                axis=0,
            )
            acc[h] = acc[h] * jnp.exp2(old - top) + jnp.dot(values, weights, preferred_element_type=F32)
            m_ref[h, 0:1] = top

    def for_step(step):
        return kv.at[jnp.where((zl + step >= 0) & (zl + step < NZL), 1, 0)]

    def right(d):
        j = 2 * d - 1
        send(for_step(d), slot(0, j, 0), z_sem.at[j], along_z(d))

    def left(d):
        j = 2 * d
        send(for_step(-d), slot(0, j, 0), z_sem.at[j], along_z(-d))

    right(1)
    left(1)
    spread(0, 0)
    right(2)
    left(2)

    def farthest():
        send(for_step(4).at[0:KROWS], slot(0, 7, 0).at[0:KROWS], z_sem.at[7], along_z(4))
        send(for_step(-4).at[KROWS:SLOT_ROWS], slot(0, 7, 0).at[KROWS:SLOT_ROWS], z_sem.at[7], along_z(-4))

    prepare_queries()
    own_chunk()
    column_event(1)
    right(3)
    left(3)
    beside_event(0)
    column_event(2)
    farthest()
    w_send(0)
    w_send(1)
    chunk(0)
    beside_event(1)
    across_event(0)
    column_event(3)
    w_send(2)
    w_send(3)
    chunk(1)
    beside_event(2)
    column_event(4)
    w_send(4)
    w_send(5)
    chunk(2)
    across_event(1)
    w_send(6)
    w_send(7)
    chunk(3)
    beside_event(3)
    chunk(4)
    across_event(2)
    beside_event(4)
    chunk(5)
    across_event(3)
    chunk(6)
    across_event(4)
    chunk(7)
    chunk(8)

    for h in range(HEADS_DEV):
        a = acc[h]
        att[:, h * HEAD : (h + 1) * HEAD] = jnp.transpose(a[0:HEAD] / a[HEAD : HEAD + 1]).astype(BF)
    send(att.at[:, 0:512], att.at[:, 512:1024], att_sem, sibling, att_sent)
    w_loaded().wait()
    arrived(wbuf.at[:, 512:1024], wx_sem.at[0])
    arrived(att.at[:, 512:1024], att_sem)

    def product(y_, zz):
        return jnp.dot(att[...], wbuf[y_ * 2 + zz], preferred_element_type=F32)

    peers = [(2, y_diag, y_over), (0, y_near, y1), (1, y_wrap, y2)]
    piece = ROWS // PIECES

    def rows(u):
        return pl.ds(u * piece, piece)

    def send_terms(n, u, cut):
        part_rows = pl.ds(u * (ROWS // cut), ROWS // cut)
        for i, _, target in peers:
            send(send1.at[n, i, part_rows], recv1.at[n, i, part_rows], r_sem.at[n, u], target, r_sent)

    for i, y_, _ in peers:
        send1[0, i] = product(y_, zo).astype(BF)
    for u in range(PIECES):
        send_terms(0, u, PIECES)
    keep[0] = product(y, zo)
    for i, y_, _ in peers:
        send1[1, i] = product(y_, zh).astype(BF)
    keep[1] = product(y, zh)

    for u in range(PIECES):
        arrived(recv1.at[0, :, rows(u)], r_sem.at[0, u])
        total = keep[0, rows(u)]
        for i in range(3):
            total = total + recv1[0, i, rows(u)].astype(F32)
        zsend[rows(u)] = total.astype(BF)
        send(zsend.at[rows(u)], zrecv.at[rows(u)], z8_sem.at[u], z_over, z8_sent)
        if u == LATE:
            send_terms(1, 0, 1)
    arrived(recv1.at[1], r_sem.at[1, 0])
    for u in range(PIECES):
        total = keep[1, rows(u)]
        for i in range(3):
            total = total + recv1[1, i, rows(u)].astype(F32)
        keep[1, rows(u)] = total
    for u in range(PIECES):
        arrived(zrecv.at[rows(u)], z8_sem.at[u])
        out_ref[rows(u)] = (keep[1, rows(u)] + zrecv[rows(u)].astype(F32)).astype(BF)

    landed(kv.at[pl.ds(0, 62)], send_sem).wait_send()
    landed(wbuf.at[:, 512:1024], wx_sem.at[1]).wait_send()
    landed(att.at[:, 0:512], att_sent).wait_send()
    landed(send1, r_sent).wait_send()
    landed(zsend, z8_sent).wait_send()


def shards(queries, keys, values, out_weight, block_order):
    any_spec = pl.BlockSpec(memory_space=pl.ANY)
    dma = pltpu.SemaphoreType.DMA
    return pl.pallas_call(
        kernel,
        out_shape=pltpu.VMEM((ROWS, ROWS), BF),
        in_specs=[any_spec] * 4 + [pl.BlockSpec(memory_space=pltpu.SMEM)],
        out_specs=pl.BlockSpec(memory_space=pltpu.VMEM),
        scratch_shapes=[
            pltpu.VMEM((SLOTS, SLOT_ROWS, HEAD), BF),
            pltpu.VMEM((3, BLK, HEAD), BF),
            pltpu.VMEM((ROWS, HEADS_DEV * HEAD), BF),
            pltpu.VMEM((HEADS_DEV, 2 * HEAD, ROWS), BF),
            pltpu.VMEM((HEADS_DEV, 8 * BLK, ROWS), F32),
            pltpu.VMEM((HEADS_DEV, 8, ROWS), F32),
            pltpu.VMEM((HEADS_DEV, HEAD + 16, ROWS), F32),
            pltpu.VMEM((ROWS, 1024), BF),
            pltpu.VMEM((8, 1024, ROWS), BF),
            pltpu.VMEM((2, ROWS, ROWS), F32),
            pltpu.VMEM((2, 3, ROWS, ROWS), BF),
            pltpu.VMEM((2, 3, ROWS, ROWS), BF),
            pltpu.VMEM((ROWS, ROWS), BF),
            pltpu.VMEM((ROWS, ROWS), BF),
            dma((7,)),
            dma,
            dma,
            dma((8,)),
            dma((5,)),
            dma((5,)),
            dma((3, 5)),
            dma((2,)),
            dma,
            dma,
            dma((2, PIECES)),
            dma,
            dma((PIECES,)),
            dma,
        ],
        compiler_params=pltpu.CompilerParams(
            collective_id=0, has_side_effects=True, vmem_limit_bytes=56 * 2**20
        ),
    )(queries, keys, values, out_weight, block_order)


def solution(mesh):
    in_specs = (P("ctx", "tp"), P("ctx", None), P("ctx", None), P("tp", None), P("ctx"))
    out_specs = P("ctx", "tp")
    return jax.shard_map(shards, mesh=mesh, in_specs=in_specs, out_specs=out_specs, check_vma=False)
```

```python
import functools
import math

import jax
import jax.numpy as jnp
from jax import lax
from jax.experimental import pallas as pl
from jax.experimental.pallas import tpu as pltpu
from jax.sharding import PartitionSpec as P

F32 = jnp.float32
BF = jnp.bfloat16
MESH = pl.DeviceIdType.MESH
HEAD = 128
BLK = 128
HEADS_DEV = 4
ROWS = 256
NX, NZL, NY = 4, 8, 4
LOG_SCALE = math.log2(math.e) / math.sqrt(HEAD)
LOW = -1e30
HIGH = 1e30

KROWS = BLK + 16
SLOT_ROWS = KROWS + HEAD
GROUPS = [[0], [1, 2], [3, 4], [5, 6], [7]]


def group(kind, p):
    side = (1, 2) if kind == "beside" else (0,) if kind == "column" else (3,)
    return [(dx, j, c) for c in (0, 1) for j in GROUPS[p] for dx in side]


CHUNKS = [
    [("beside", 0), ("column", 1)],
    [("beside", 1)],
    [("across", 0), ("column", 2)],
    [("beside", 2)],
    [("across", 1), ("column", 3)],
    [("beside", 3)],
    [("across", 2), ("column", 4)],
    [("beside", 4), ("across", 3)],
    [("across", 4)],
]
SLOT = {(0, 0, 0): 1, (0, 0, 1): 2}
SPANS = []
for parts in CHUNKS:
    first = len(SLOT) + 1
    for part in parts:
        for name in group(*part):
            SLOT[name] = len(SLOT) + 1
    SPANS.append((first, len(SLOT) + 1 - first))
SLOTS = len(SLOT) + 1
PIECES = 8
LATE = 3
RELAYED = (0, 1, 2, 3)


def kernel(
    q_hbm, k_hbm, v_hbm, w_hbm, order_ref, out_ref,
    kv, vtmp, q_ref, qt, s_ref, m_ref, acc, att, wbuf,
    keep, send1, recv1, zsend, zrecv,
    load_sem, w_sem, send_sem, z_sem, x_sem, x2_sem, sib_sem, wx_sem, att_sem, att_sent, r_sem, r_sent, z8_sem, z8_sent,
):
    ctx = lax.axis_index("ctx")
    tp = lax.axis_index("tp")
    x, zl = ctx // NZL, ctx % NZL
    y, zh, core = tp // 4, (tp // 2) % 2, tp % 2
    zo = 1 - zh
    head = tp // 2
    far_head = y * 2 + zo

    def device(x_=None, zl_=None, y_=None, zh_=None, core_=None):
        x_ = x if x_ is None else x_
        zl_ = zl if zl_ is None else zl_
        y_ = y if y_ is None else y_
        zh_ = zh if zh_ is None else zh_
        core_ = core if core_ is None else core_
        return {"ctx": x_ * NZL + zl_, "tp": y_ * 4 + zh_ * 2 + core_}

    def along_z(step):
        z = (zh * NZL + zl + step + 2 * NZL) % (2 * NZL)
        return device(zl_=z % NZL, zh_=z // NZL)

    sibling = device(core_=1 - core)
    x_over, z_over = device(x_=(x + 2) % NX), device(zh_=zo)
    x_up, x_down = device(x_=(x + 1) % NX), device(x_=(x + NX - 1) % NX)
    y_near = y + 1 - 2 * (y % 2)
    y_wrap = NY - 1 - y
    y_diag = (y + 2) % NY
    y1, y2, y_over = device(y_=y_near), device(y_=y_wrap), device(y_=y_diag)

    barrier = pltpu.get_barrier_semaphore()
    friends = [sibling, x_up, x_down, x_over, y1, y2, y_over]
    friends += [along_z(s) for s in (1, -1, 2, -2)]
    for friend in friends:
        pl.semaphore_signal(barrier, inc=1, device_id=friend, device_id_type=MESH)

    mine = pl.ds(pl.multiple_of(core * BLK, BLK), BLK)
    other = pl.ds(pl.multiple_of((1 - core) * BLK, BLK), BLK)
    own_cols = pl.ds(pl.multiple_of(head * HEAD, HEAD), HEAD)
    far_cols = pl.ds(pl.multiple_of(far_head * HEAD, HEAD), HEAD)
    loads = [
        pltpu.make_async_copy(v_hbm.at[mine, own_cols], vtmp.at[0], load_sem.at[0]),
        pltpu.make_async_copy(v_hbm.at[mine, far_cols], vtmp.at[1], load_sem.at[1]),
        pltpu.make_async_copy(v_hbm.at[other, own_cols], vtmp.at[2], load_sem.at[2]),
        pltpu.make_async_copy(k_hbm.at[mine, own_cols], kv.at[1, 0:BLK], load_sem.at[3]),
        pltpu.make_async_copy(k_hbm.at[mine, far_cols], kv.at[0, 0:BLK], load_sem.at[4]),
        pltpu.make_async_copy(k_hbm.at[other, own_cols], kv.at[2, 0:BLK], load_sem.at[5]),
        pltpu.make_async_copy(q_hbm, q_ref, load_sem.at[6]),
    ]
    for load in loads:
        load.start()

    def w_cols(q, core_):
        return pl.ds(pl.multiple_of((q * 2 + core_) * ROWS, ROWS), ROWS)

    def w_loaded():
        whole = wbuf.at[:, 0:512]
        return pltpu.make_async_copy(whole, whole, w_sem)

    place = [order_ref[0].astype(F32), order_ref[1].astype(F32)]
    my_place = order_ref[core].astype(F32)
    other_place = order_ref[1 - core].astype(F32)

    def transposed(v):
        return jnp.transpose(v.astype(F32)).astype(BF)

    for i, (which, load) in enumerate([(my_place, 1), (my_place, 0), (other_place, 2)]):
        kv[load, BLK:KROWS] = jnp.full((16, HEAD), which, F32).astype(BF)
        loads[i].wait()
        kv[load, KROWS:SLOT_ROWS] = transposed(vtmp[i])
    for load in loads[3:]:
        load.wait()
    for q in range(8):
        pltpu.make_async_copy(w_hbm.at[:, w_cols(q, core)], wbuf.at[q, 0:512], w_sem).start()
    pl.semaphore_wait(barrier, len(friends))

    def send(src, dst, recv, target, sent=None):
        pltpu.make_async_remote_copy(
            src_ref=src, dst_ref=dst, send_sem=send_sem if sent is None else sent, recv_sem=recv,
            device_id=target, device_id_type=MESH,
        ).start()

    def landed(ref, sem):
        return pltpu.make_async_remote_copy(
            src_ref=ref, dst_ref=ref, send_sem=sem, recv_sem=sem, device_id=sibling, device_id_type=MESH
        )

    def arrived(ref, sem):
        landed(ref, sem).wait_recv()

    def slot(dx, j, c):
        return kv.at[SLOT[(dx, j, c)]]

    def part(kind, p, c):
        names = group(kind, p)
        count = len(names) // 2
        return kv.at[pl.ds(SLOT[names[c * count]], count)]

    KINDS = {"column": 0, "beside": 1, "across": 2}

    def spread(p, j):
        send(slot(0, j, 0), slot(1, j, 0), x_sem.at[p], x_up)
        send(slot(0, j, 0), slot(2, j, 0), x_sem.at[p], x_down)
        if p not in RELAYED:
            send(slot(0, j, 0), slot(3, j, 0), x2_sem.at[p], x_over)

    def share(kind, p):
        send(part(kind, p, 0), part(kind, p, 1), sib_sem.at[KINDS[kind], p], sibling)

    def column_event(p):
        for j in GROUPS[p]:
            arrived(slot(0, j, 0), z_sem.at[j])
            spread(p, j)
        share("column", p)

    def beside_event(p):
        arrived(part("beside", p, 0), x_sem.at[p])
        if p in RELAYED:
            for j in GROUPS[p]:
                keys, values = pl.ds(0, KROWS), pl.ds(KROWS, HEAD)
                send(slot(1, j, 0).at[keys], slot(3, j, 0).at[keys], x2_sem.at[p], x_up)
                send(slot(2, j, 0).at[values], slot(3, j, 0).at[values], x2_sem.at[p], x_down)
        share("beside", p)

    def across_event(p):
        arrived(part("across", p, 0), x2_sem.at[p])
        share("across", p)

    def w_send(q):
        send(w_hbm.at[:, w_cols(q, 1 - core)], wbuf.at[q, 512:1024], wx_sem.at[0], sibling, wx_sem.at[1])

    def prepare_queries():
        for h in range(HEADS_DEV):
            t = jnp.transpose(q_ref[:, h * HEAD : (h + 1) * HEAD].astype(F32)) * LOG_SCALE
            top = t.astype(BF)
            qt[h, 0:HEAD] = top
            qt[h, HEAD : 2 * HEAD] = (t - top.astype(F32)).astype(BF)

    q_place = jnp.concatenate([jnp.full((1, BLK), place[0], F32), jnp.full((1, BLK), place[1], F32)], axis=1)

    def keys_values(base, count):
        ks, vs = [], []
        for i in range(count):
            k = kv[base + i, 0:BLK]
            ks.append(jnp.concatenate([k, k], axis=1))
            vs.append(kv[base + i, KROWS:SLOT_ROWS])
        values = jnp.concatenate([jnp.concatenate(vs, axis=1), jnp.ones((16, count * BLK), BF)], axis=0)
        return jnp.concatenate(ks, axis=0), values

    def own_chunk():
        keys, values = keys_values(1, 2)
        rows = lax.broadcasted_iota(jnp.int32, (BLK, ROWS), 0).astype(F32)
        lanes = (lax.broadcasted_iota(jnp.int32, (1, ROWS), 1) % BLK).astype(F32)
        q_pos = q_place * BLK + lanes
        seen = [rows + my_place * BLK <= q_pos, rows + other_place * BLK <= q_pos]
        for h in range(HEADS_DEV):
            s = jnp.dot(keys, qt[h], preferred_element_type=F32)
            parts = [jnp.where(seen[i], s[i * BLK : (i + 1) * BLK], LOW) for i in range(2)]
            top = jnp.maximum(
                jnp.max(parts[0], axis=0, keepdims=True), jnp.max(parts[1], axis=0, keepdims=True)
            )
            weights = jnp.concatenate([jnp.exp2(part - top).astype(BF) for part in parts], axis=0)
            acc[h] = jnp.dot(values, weights, preferred_element_type=F32)
            m_ref[h, 0:1] = top

    def chunk(n):
        base, count = SPANS[n]
        for kind, p in CHUNKS[n]:
            arrived(part(kind, p, 1), sib_sem.at[KINDS[kind], p])
        keys, values = keys_values(base, count)
        seen = []
        for i in range(count):
            p = kv[base + i, BLK:KROWS].astype(F32)[0:1]
            seen.append(jnp.concatenate([p, p], axis=1) < q_place)
        for h in range(HEADS_DEV):
            s_ref[h, 0 : count * BLK] = jnp.dot(keys, qt[h], preferred_element_type=F32)
        for h in range(HEADS_DEV):
            old = m_ref[h, 0:1]
            top = old
            for i in range(count):
                high = jnp.max(s_ref[h, i * BLK : (i + 1) * BLK], axis=0, keepdims=True)
                top = jnp.maximum(top, jnp.where(seen[i], high, LOW))
            weights = jnp.concatenate(
                [
                    jnp.exp2(s_ref[h, i * BLK : (i + 1) * BLK] - jnp.where(seen[i], top, HIGH)).astype(BF)
                    for i in range(count)
                ],
                axis=0,
            )
            acc[h] = acc[h] * jnp.exp2(old - top) + jnp.dot(values, weights, preferred_element_type=F32)
            m_ref[h, 0:1] = top

    def for_step(step):
        return kv.at[jnp.where((zl + step >= 0) & (zl + step < NZL), 1, 0)]

    def right(d):
        j = 2 * d - 1
        send(for_step(d), slot(0, j, 0), z_sem.at[j], along_z(d))

    def left(d):
        j = 2 * d
        send(for_step(-d), slot(0, j, 0), z_sem.at[j], along_z(-d))

    right(1)
    left(1)
    spread(0, 0)
    right(2)
    left(2)

    def farthest():
        send(for_step(4).at[0:KROWS], slot(0, 7, 0).at[0:KROWS], z_sem.at[7], along_z(4))
        send(for_step(-4).at[KROWS:SLOT_ROWS], slot(0, 7, 0).at[KROWS:SLOT_ROWS], z_sem.at[7], along_z(-4))

    prepare_queries()
    column_event(1)
    right(3)
    left(3)
    beside_event(0)
    own_chunk()
    column_event(2)
    farthest()
    w_send(0)
    w_send(1)
    chunk(0)
    beside_event(1)
    across_event(0)
    column_event(3)
    w_send(2)
    w_send(3)
    chunk(1)
    beside_event(2)
    column_event(4)
    w_send(4)
    w_send(5)
    chunk(2)
    across_event(1)
    w_send(6)
    w_send(7)
    chunk(3)
    beside_event(3)
    chunk(4)
    across_event(2)
    beside_event(4)
    chunk(5)
    across_event(3)
    chunk(6)
    across_event(4)
    chunk(7)
    chunk(8)

    for h in range(HEADS_DEV):
        a = acc[h]
        att[:, h * HEAD : (h + 1) * HEAD] = jnp.transpose(a[0:HEAD] / a[HEAD : HEAD + 1]).astype(BF)
    send(att.at[:, 0:512], att.at[:, 512:1024], att_sem, sibling, att_sent)
    w_loaded().wait()
    arrived(wbuf.at[:, 512:1024], wx_sem.at[0])
    arrived(att.at[:, 512:1024], att_sem)

    def product(y_, zz):
        return jnp.dot(att[...], wbuf[y_ * 2 + zz], preferred_element_type=F32)

    peers = [(2, y_diag, y_over), (0, y_near, y1), (1, y_wrap, y2)]
    piece = ROWS // PIECES

    def rows(u):
        return pl.ds(u * piece, piece)

    def send_terms(n, u, cut):
        part_rows = pl.ds(u * (ROWS // cut), ROWS // cut)
        for i, _, target in peers:
            send(send1.at[n, i, part_rows], recv1.at[n, i, part_rows], r_sem.at[n, u], target, r_sent)

    for i, y_, _ in peers:
        send1[0, i] = product(y_, zo).astype(BF)
    for u in range(PIECES):
        send_terms(0, u, PIECES)
    keep[0] = product(y, zo)
    for i, y_, _ in peers:
        send1[1, i] = product(y_, zh).astype(BF)
    keep[1] = product(y, zh)

    for u in range(PIECES):
        arrived(recv1.at[0, :, rows(u)], r_sem.at[0, u])
        total = keep[0, rows(u)]
        for i in range(3):
            total = total + recv1[0, i, rows(u)].astype(F32)
        zsend[rows(u)] = total.astype(BF)
        send(zsend.at[rows(u)], zrecv.at[rows(u)], z8_sem.at[u], z_over, z8_sent)
        if u == LATE:
            send_terms(1, 0, 1)
    arrived(recv1.at[1], r_sem.at[1, 0])
    for u in range(PIECES):
        total = keep[1, rows(u)]
        for i in range(3):
            total = total + recv1[1, i, rows(u)].astype(F32)
        keep[1, rows(u)] = total
    for u in range(PIECES):
        arrived(zrecv.at[rows(u)], z8_sem.at[u])
        out_ref[rows(u)] = (keep[1, rows(u)] + zrecv[rows(u)].astype(F32)).astype(BF)

    landed(kv.at[pl.ds(0, 62)], send_sem).wait_send()
    landed(wbuf.at[:, 512:1024], wx_sem.at[1]).wait_send()
    landed(att.at[:, 0:512], att_sent).wait_send()
    landed(send1, r_sent).wait_send()
    landed(zsend, z8_sent).wait_send()


def shards(queries, keys, values, out_weight, block_order):
    any_spec = pl.BlockSpec(memory_space=pl.ANY)
    dma = pltpu.SemaphoreType.DMA
    return pl.pallas_call(
        kernel,
        out_shape=pltpu.VMEM((ROWS, ROWS), BF),
        in_specs=[any_spec] * 4 + [pl.BlockSpec(memory_space=pltpu.SMEM)],
        out_specs=pl.BlockSpec(memory_space=pltpu.VMEM),
        scratch_shapes=[
            pltpu.VMEM((SLOTS, SLOT_ROWS, HEAD), BF),
            pltpu.VMEM((3, BLK, HEAD), BF),
            pltpu.VMEM((ROWS, HEADS_DEV * HEAD), BF),
            pltpu.VMEM((HEADS_DEV, 2 * HEAD, ROWS), BF),
            pltpu.VMEM((HEADS_DEV, 8 * BLK, ROWS), F32),
            pltpu.VMEM((HEADS_DEV, 8, ROWS), F32),
            pltpu.VMEM((HEADS_DEV, HEAD + 16, ROWS), F32),
            pltpu.VMEM((ROWS, 1024), BF),
            pltpu.VMEM((8, 1024, ROWS), BF),
            pltpu.VMEM((2, ROWS, ROWS), F32),
            pltpu.VMEM((2, 3, ROWS, ROWS), BF),
            pltpu.VMEM((2, 3, ROWS, ROWS), BF),
            pltpu.VMEM((ROWS, ROWS), BF),
            pltpu.VMEM((ROWS, ROWS), BF),
            dma((7,)),
            dma,
            dma,
            dma((8,)),
            dma((5,)),
            dma((5,)),
            dma((3, 5)),
            dma((2,)),
            dma,
            dma,
            dma((2, PIECES)),
            dma,
            dma((PIECES,)),
            dma,
        ],
        compiler_params=pltpu.CompilerParams(
            collective_id=0, has_side_effects=True, vmem_limit_bytes=56 * 2**20
        ),
    )(queries, keys, values, out_weight, block_order)


def solution(mesh):
    in_specs = (P("ctx", "tp"), P("ctx", None), P("ctx", None), P("tp", None), P("ctx"))
    out_specs = P("ctx", "tp")
    return jax.shard_map(shards, mesh=mesh, in_specs=in_specs, out_specs=out_specs, check_vma=False)
```
